32 devices in a mesh: ty: 16 (over z, y, core), tx: 2 (over x).
Axes of the slice: x: 2, y: 2, z: 4, core: 2. Of those that a mesh axis runs over, the one named last changes fastest.
Arguments:
- ctrl: float32 [16, 2, 512, 640], P('ty', 'tx'), may hold values from -6 to 6
- interp_wt: float32 [16, 2, 4, 128, 384], P('ty', 'tx'), may hold values from -0.3125 to 0.3125
- interp_cols: int32 [16, 2, 4, 384], P('ty', 'tx'), may hold values from 0 to 1023
- conv_wt: float32 [16, 2, 4, 128, 512], P('ty', 'tx'), may hold values from -0.25 to 0.25
- conv_cols: int32 [16, 2, 4, 512], P('ty', 'tx'), may hold values from 0 to 1023
- halo_index: int32 [16, 2, 8, 64], P('ty', 'tx'), may hold values from 0 to 511
- valid: int32 [16, 2], P('ty', 'tx'), may hold values from 256 to 512
Outputs:
- localized: float32 [16, 2, 512, 640], P('ty', 'tx')
The draws below stay inside these ranges and needn't reach their ends.
Inputs may be any that keep to these rules, and one draw needn't show every extreme that they name: `interp_cols`: indices into a tile's extended subgrid of 1024 rows; repeats are allowed. `conv_cols`: indices into a tile's extended subgrid; repeats are allowed. `halo_index`: owned row indices; repeats are allowed.
All inputs are finite; a program needn't handle non-finite values.
Results may differ from the reference program's by a relative error of at most 0.0001.
Values sent between devices are 32-bit elements; how exact they have to be, the bound alone decides.
A program may use at most 64 MiB of HBM per device.

```python
import jax
import jax.numpy as jnp
from jax import lax

NODES = 512
GRID = 512
HALO = 64
GROWS = 128
GCOLS = 384
CROWS = 128
CCOLS = 512
FEAT = 640
EXT = 1024
GBLK = 4
CBLK = 4
N_TY = 16
N_TX = 2


def with_ends(array, key, smallest, top_value):
    longest = array.shape.index(max(array.shape))
    spots = []
    for shift in (0, 1):
        where = [jax.random.randint(jax.random.fold_in(key, axis), (), 0, length) for axis, length in enumerate(array.shape)]
        where[longest] = (where[longest] + shift) % array.shape[longest]
        spots.append(tuple(where))
    return array.at[spots[0]].set(smallest).at[spots[1]].set(top_value)


def steps_of(stream_key, dims, cuts, low, largest):
    gain, own = 1.0, jax.random.fold_in(stream_key, 6)
    for position, blocks in cuts:
        steps = jnp.exp(jax.random.uniform(jax.random.fold_in(own, position), (blocks,), jnp.float32, low / len(cuts), largest / len(cuts)))
        gain = gain * jnp.repeat(steps, dims[position] // blocks).reshape([-1 if axis == position else 1 for axis in range(len(dims))])
    return gain


def scatter_about(rng, shape, scale, most, cuts=(), kind=jnp.bfloat16):
    gain = steps_of(rng, shape, cuts, -0.22, 0.18) if cuts else 1.0
    values = jax.random.normal(rng, shape, jnp.float32) * scale * gain
    return jnp.minimum(jnp.maximum(values, -most), most).astype(kind)


def setup_inputs(seed: int = 0) -> dict:
    keys = jax.random.split(jax.random.key(seed), 8)
    return {
        "ctrl": scatter_about(keys[0], (N_TY, N_TX, GRID, FEAT), 1.0, 6.0, ((0, 16), (1, 2)), jnp.float32),
        "interp_wt": scatter_about(keys[1], (N_TY, N_TX, GBLK, GROWS, GCOLS), GCOLS ** -0.5, 0.3125, ((0, 16), (1, 2)), jnp.float32),
        "interp_cols": with_ends(jax.random.randint(keys[2], (N_TY, N_TX, GBLK, GCOLS), 0, EXT), jax.random.fold_in(keys[2], 1), 0, EXT - 1).astype(jnp.int32),
        "conv_wt": scatter_about(keys[3], (N_TY, N_TX, CBLK, CROWS, CCOLS), CCOLS ** -0.5, 0.25, ((0, 16), (1, 2)), jnp.float32),
        "conv_cols": with_ends(jax.random.randint(keys[4], (N_TY, N_TX, CBLK, CCOLS), 0, EXT), jax.random.fold_in(keys[4], 1), 0, EXT - 1).astype(jnp.int32),
        "halo_index": with_ends(jax.random.randint(keys[5], (N_TY, N_TX, 8, HALO), 0, NODES), jax.random.fold_in(keys[5], 1), 0, NODES - 1).astype(jnp.int32),
        "valid": with_ends(jax.random.randint(keys[6], (N_TY, N_TX), GRID // 2, GRID + 1), jax.random.fold_in(keys[6], 1), GRID // 2, GRID).astype(jnp.int32),
    }


DIRECTIONS = ((-1, -1), (-1, 0), (-1, 1), (0, -1), (0, 1), (1, -1), (1, 0), (1, 1))


def neighbour(tiles, row_off, col_off):
    shifted = jnp.roll(tiles, -col_off, axis=1)
    edge = jnp.zeros_like(shifted[:1])
    if row_off == 1:
        return jnp.concatenate([shifted[1:], edge], axis=0)
    if row_off == -1:
        return jnp.concatenate([edge, shifted[:-1]], axis=0)
    return shifted


def over_tiles(func, *arrays):
    rows_t, cols_t = arrays[0].shape[:2]
    flat = tuple(item.reshape((rows_t * cols_t,) + item.shape[2:]) for item in arrays)
    result = lax.map(lambda packed: func(*packed), flat)
    return result.reshape((rows_t, cols_t) + result.shape[1:])


def forward_blocks(weights, cols, source):
    gathered = jnp.take(source, cols, axis=0)
    result = jnp.einsum("bgc,bcf->bgf", weights, gathered, precision=lax.Precision.HIGHEST)
    return result.reshape(-1, source.shape[1])


def adjoint_blocks(weights, cols, values):
    blocks = values.reshape(weights.shape[0], weights.shape[1], values.shape[1])
    contrib = jnp.einsum("bgc,bgf->bcf", weights, blocks, precision=lax.Precision.HIGHEST)
    return jax.ops.segment_sum(contrib.reshape(-1, values.shape[1]), cols.reshape(-1), num_segments=EXT)


def accumulate(contrib, halo_index):
    owned = contrib[:, :, :NODES]
    slots = contrib[:, :, NODES:].reshape(contrib.shape[0], contrib.shape[1], 8, HALO, FEAT)
    for slot_id in range(8):
        row_off, col_off = DIRECTIONS[slot_id]
        arrived = neighbour(slots[:, :, slot_id], row_off, col_off)
        owned = owned + over_tiles(lambda vals, idx: jax.ops.segment_sum(vals, idx, num_segments=NODES), arrived, halo_index[:, :, slot_id])
    return owned


def extend(owned, halo_index):
    sends = over_tiles(lambda field, idx: jnp.take(field, idx, axis=0), owned, halo_index)
    slots = []
    for slot_id in range(8):
        row_off, col_off = DIRECTIONS[slot_id]
        slots.append(neighbour(sends[:, :, slot_id], -row_off, -col_off))
    stacked = jnp.stack(slots, axis=2).reshape(owned.shape[0], owned.shape[1], 8 * HALO, FEAT)
    return jnp.concatenate([owned, stacked], axis=2)


def reference(ctrl, interp_wt, interp_cols, conv_wt, conv_cols, halo_index, valid):
    positions = jnp.arange(GRID, dtype=jnp.int32)
    mask = (positions[None, None, :] < valid[:, :, None]).astype(jnp.float32)[..., None]
    masked = ctrl * mask
    a_ext = over_tiles(adjoint_blocks, interp_wt, interp_cols, masked)
    summed = accumulate(a_ext, halo_index)
    b_ext = over_tiles(adjoint_blocks, conv_wt, conv_cols, summed)
    spread = accumulate(b_ext, halo_index)
    smooth = over_tiles(forward_blocks, conv_wt, conv_cols, extend(spread, halo_index))
    result = over_tiles(forward_blocks, interp_wt, interp_cols, extend(smooth, halo_index))
    return result * mask
```

```python
import functools

import jax
import jax.numpy as jnp
from jax import lax
from jax.experimental import pallas as pl
from jax.experimental.pallas import tpu as pltpu
from jax.sharding import PartitionSpec as P

MESH = pl.DeviceIdType.MESH
DIRECTIONS = ((-1, -1), (-1, 0), (-1, 1), (0, -1), (0, 1), (1, -1), (1, 0), (1, 1))
ORDER = (0, 2, 5, 7, 3, 4, 1, 6)
F32, BF16 = jnp.float32, jnp.bfloat16


def halves(x):
    hi = x.astype(BF16)
    return hi, (x - hi.astype(F32)).astype(BF16)


def dot(a, b):
    return jnp.dot(a, b, preferred_element_type=F32)


def dot_nt(a, b):
    return lax.dot_general(a, b, (((1,), (1,)), ((), ())), preferred_element_type=F32)


def kernel(
    n_ty, n_tx, chunks, valid_ref, ctrl_ref, iwt_ref, icols_ref, cwt_ref, ccols_ref, halo_ref,
    out_ref, imat, imat_t, cmat, cmat_t, pick, pick_t, *rest,
):
    n_chunks = len(chunks)
    send_sem, recv_sem = rest[-2:]
    buffers = rest[:-2]
    own = buffers[:n_chunks]
    rhs = buffers[n_chunks : 2 * n_chunks]
    send = [buffers[(2 + e) * n_chunks : (3 + e) * n_chunks] for e in range(4)]
    recv = [buffers[(6 + e) * n_chunks : (7 + e) * n_chunks] for e in range(4)]
    ty, tx = lax.axis_index("ty"), lax.axis_index("tx")
    rows = out_ref.shape[0]
    n_own = own[0].shape[0]
    n_slot = recv[0][0].shape[0]
    slot = n_slot // 8
    extent = n_own + n_slot

    def there(off):
        return jnp.logical_and(ty + off >= 0, ty + off < n_ty)

    def peer(row_off, col_off):
        return ty + row_off, lax.rem(tx + col_off + n_tx, n_tx)

    barrier = pltpu.get_barrier_semaphore()
    for row_off, col_off in DIRECTIONS:
        @pl.when(there(row_off))
        def _():
            pl.semaphore_signal(
                barrier, inc=1, device_id=peer(row_off, col_off), device_id_type=MESH
            )

    def copy(e, c, d):
        sign = -1 if e < 2 else 1
        row_off, col_off = DIRECTIONS[d]
        piece = pl.ds(d * slot, slot)
        return pltpu.make_async_remote_copy(
            src_ref=send[e][c].at[piece],
            dst_ref=recv[e][c].at[piece],
            send_sem=send_sem.at[e, c, d],
            recv_sem=recv_sem.at[e, c, d],
            device_id=peer(sign * row_off, sign * col_off),
            device_id_type=MESH,
        )

    def each(e, c, sending, action):
        sign = -1 if e < 2 else 1
        for d in ORDER:
            row_off = DIRECTIONS[d][0] * (sign if sending else -sign)
            if row_off == 0:
                action(copy(e, c, d))
            else:
                pl.when(there(row_off))(functools.partial(lambda e, c, d: action(copy(e, c, d)), e, c, d))

    def start(e, c):
        each(e, c, True, lambda item: item.start())

    def arrived(e, c):
        each(e, c, False, lambda item: item.wait_recv())

    def spread(wt_ref, cols_ref, mat, mat_t):
        blocks, height, width = wt_ref.shape
        for b in range(blocks):
            index = cols_ref[b : b + 1, :]
            hot = (lax.broadcasted_iota(jnp.int32, (extent, width), 0) == index).astype(F32).astype(BF16)
            hi, lo = halves(wt_ref[b])
            span = pl.ds(b * height, height)
            if mat is not None:
                mat[0, span], mat[1, span] = halves(dot_nt(hi, hot) + dot_nt(lo, hot))
            if mat_t is not None:
                mat_t[0, :, span], mat_t[1, :, span] = halves(dot_nt(hot, hi) + dot_nt(hot, lo))

    def product(mat, row0, count, col0, depth, c, base):
        a_hi = mat[0, row0 : row0 + count, col0 : col0 + depth]
        a_lo = mat[1, row0 : row0 + count, col0 : col0 + depth]
        b_hi, b_lo = rhs[c][0, base : base + depth], rhs[c][1, base : base + depth]
        return dot(a_hi, b_hi) + (dot(a_hi, b_lo) + dot(a_lo, b_hi))

    def gathered(e, c):
        hi, lo = halves(recv[e][c][...])
        return dot(pick_t[...], hi) + dot(pick_t[...], lo)

    def place(c, base, value):
        rhs[c][0, base : base + value.shape[0]], rhs[c][1, base : base + value.shape[0]] = halves(value)

    def picked(c):
        return dot(pick[...], rhs[c][0, :n_own]) + dot(pick[...], rhs[c][1, :n_own])

    for e in range(4):
        sign = -1 if e < 2 else 1
        for d, (row_off, _) in enumerate(DIRECTIONS):
            if row_off:
                @pl.when(jnp.logical_not(there(-sign * row_off)))
                def _():
                    for c in range(n_chunks):
                        piece = recv[e][c].at[pl.ds(d * slot, slot)]
                        piece[...] = jnp.zeros(piece.shape, F32)

    spread(iwt_ref, icols_ref, None, imat_t)
    limit = valid_ref[0, 0]
    edge = jnp.int32(2)
    edge += jnp.where(there(-1), 3, 0) + jnp.where(there(1), 3, 0)
    pl.semaphore_wait(barrier, edge)

    def keep(width):
        return lax.broadcasted_iota(jnp.int32, (rows, width), 0) < limit

    for c, (lo, width) in enumerate(chunks):
        place(c, 0, jnp.where(keep(width), ctrl_ref[:, lo : lo + width], 0.0))
        send[0][c][...] = product(imat_t, n_own, n_slot, 0, rows, c, 0)
        start(0, c)
        own[c][...] = product(imat_t, 0, n_own, 0, rows, c, 0)
    hot = (lax.broadcasted_iota(jnp.int32, (n_own, n_slot), 0) == halo_ref[...]).astype(F32)
    pick_t[...] = hot.astype(BF16)
    pick[...] = hot.T.astype(BF16)
    spread(cwt_ref, ccols_ref, None, cmat_t)
    for c in range(n_chunks):
        arrived(0, c)
        place(c, 0, own[c][...] + gathered(0, c))
        send[1][c][...] = product(cmat_t, n_own, n_slot, 0, n_own, c, 0)
        start(1, c)
        own[c][...] = product(cmat_t, 0, n_own, 0, n_own, c, 0)
    spread(cwt_ref, ccols_ref, cmat, None)
    spread(iwt_ref, icols_ref, imat, None)
    for c in range(n_chunks):
        arrived(1, c)
        place(c, 0, own[c][...] + gathered(1, c))
        send[2][c][...] = picked(c)
        start(2, c)
        own[c][...] = product(cmat, 0, n_own, 0, n_own, c, 0)
    for c in range(n_chunks):
        arrived(2, c)
        place(c, n_own, recv[2][c][...])
        place(c, 0, own[c][...] + product(cmat, 0, n_own, n_own, n_slot, c, n_own))
        send[3][c][...] = picked(c)
        start(3, c)
        own[c][...] = product(imat, 0, rows, 0, n_own, c, 0)
    for c, (lo, width) in enumerate(chunks):
        arrived(3, c)
        place(c, n_own, recv[3][c][...])
        total = own[c][...] + product(imat, 0, rows, n_own, n_slot, c, n_own)
        out_ref[:, lo : lo + width] = jnp.where(keep(width), total, 0.0)
    for e in range(4):
        for c in range(n_chunks):
            each(e, c, True, lambda item: item.wait_send())


def solution(mesh):
    n_ty, n_tx = mesh.shape["ty"], mesh.shape["tx"]

    def body(ctrl, interp_wt, interp_cols, conv_wt, conv_cols, halo_index, valid):
        rows, feat = ctrl.shape[2:]
        n_own = conv_wt.shape[2] * conv_wt.shape[3]
        n_slot = halo_index.shape[2] * halo_index.shape[3]
        extent = n_own + n_slot
        tiles = feat // 128
        first = 128 * max(tiles // 2, 1)
        chunks = ((0, first), (first, feat - first)) if feat > first else ((0, feat),)
        widths = [width for _, width in chunks]
        vmem = pl.BlockSpec(memory_space=pltpu.VMEM)
        scratch = [
            pltpu.VMEM((2, rows, extent), BF16),
            pltpu.VMEM((2, extent, rows), BF16),
            pltpu.VMEM((2, n_own, extent), BF16),
            pltpu.VMEM((2, extent, n_own), BF16),
            pltpu.VMEM((n_slot, n_own), BF16),
            pltpu.VMEM((n_own, n_slot), BF16),
        ]
        scratch += [pltpu.VMEM((n_own, width), F32) for width in widths]
        scratch += [pltpu.VMEM((2, extent, width), BF16) for width in widths]
        scratch += [pltpu.VMEM((n_slot, width), F32) for _ in range(8) for width in widths]
        scratch += [pltpu.SemaphoreType.DMA((4, len(chunks), 8))] * 2
        out = pl.pallas_call(
            functools.partial(kernel, n_ty, n_tx, chunks),
            out_shape=jax.ShapeDtypeStruct((rows, feat), F32),
            in_specs=[pl.BlockSpec(memory_space=pltpu.SMEM)] + [vmem] * 6,
            out_specs=vmem,
            scratch_shapes=scratch,
            compiler_params=pltpu.CompilerParams(
                collective_id=0, has_side_effects=True, vmem_limit_bytes=60 * 1024 * 1024
            ),
        )(
            valid, ctrl[0, 0], interp_wt[0, 0], interp_cols[0, 0], conv_wt[0, 0], conv_cols[0, 0],
            halo_index.reshape(1, n_slot),
        )
        return out[None, None]

    placed = (
        P("ty", "tx", None, None),
        P("ty", "tx", None, None, None),
        P("ty", "tx", None, None),
        P("ty", "tx", None, None, None),
        P("ty", "tx", None, None),
        P("ty", "tx", None, None),
        P("ty", "tx"),
    )
    return jax.shard_map(
        body, mesh=mesh, in_specs=placed, out_specs=P("ty", "tx", None, None), check_vma=False
    )
```

```python
import functools

import jax
import jax.numpy as jnp
from jax import lax
from jax.experimental import pallas as pl
from jax.experimental.pallas import tpu as pltpu
from jax.sharding import PartitionSpec as P

MESH = pl.DeviceIdType.MESH
DIRECTIONS = ((-1, -1), (-1, 0), (-1, 1), (0, -1), (0, 1), (1, -1), (1, 0), (1, 1))
ORDER = (0, 2, 5, 7, 3, 4, 1, 6)
F32, BF16 = jnp.float32, jnp.bfloat16


def halves(x):
    hi = x.astype(BF16)
    return hi, (x - hi.astype(F32)).astype(BF16)


def dot(a, b):
    return jnp.dot(a, b, preferred_element_type=F32)


def dot_nt(a, b):
    return lax.dot_general(a, b, (((1,), (1,)), ((), ())), preferred_element_type=F32)


def kernel(
    n_ty, n_tx, chunks, valid_ref, ctrl_hbm, iwt_hbm, icols_ref, cwt_hbm, ccols_ref, halo_ref,
    out_ref, iwt_ref, cwt_ref, imat, imat_t, cmat, cmat_t, pick, pick_t, *rest,
):
    n_chunks = len(chunks)
    send_sem, recv_sem, load_sem, store_sem = rest[-4:]
    buffers = rest[:-4]
    own = buffers[:n_chunks]
    rhs = buffers[n_chunks : 2 * n_chunks]
    send = [buffers[(2 + e) * n_chunks : (3 + e) * n_chunks] for e in range(4)]
    recv = [buffers[(6 + e) * n_chunks : (7 + e) * n_chunks] for e in range(4)]
    loads = [pltpu.make_async_copy(iwt_hbm, iwt_ref, load_sem.at[0])]
    for c, (lo, width) in enumerate(chunks):
        loads.append(
            pltpu.make_async_copy(ctrl_hbm.at[:, lo : lo + width], own[c], load_sem.at[1 + c])
        )
    loads.append(pltpu.make_async_copy(cwt_hbm, cwt_ref, load_sem.at[1 + n_chunks]))
    for item in loads:
        item.start()
    ty, tx = lax.axis_index("ty"), lax.axis_index("tx")
    rows = out_ref.shape[0]
    n_own = own[0].shape[0]
    n_slot = recv[0][0].shape[0]
    slot = n_slot // 8
    extent = n_own + n_slot

    def there(off):
        return jnp.logical_and(ty + off >= 0, ty + off < n_ty)

    def peer(row_off, col_off):
        return ty + row_off, lax.rem(tx + col_off + n_tx, n_tx)

    barrier = pltpu.get_barrier_semaphore()
    for row_off, col_off in DIRECTIONS:
        @pl.when(there(row_off))
        def _():
            pl.semaphore_signal(
                barrier, inc=1, device_id=peer(row_off, col_off), device_id_type=MESH
            )

    def copy(e, c, d):
        sign = -1 if e < 2 else 1
        row_off, col_off = DIRECTIONS[d]
        piece = pl.ds(d * slot, slot)
        return pltpu.make_async_remote_copy(
            src_ref=send[e][c].at[piece],
            dst_ref=recv[e][c].at[piece],
            send_sem=send_sem.at[e, c, d],
            recv_sem=recv_sem.at[e, c, d],
            device_id=peer(sign * row_off, sign * col_off),
            device_id_type=MESH,
        )

    def each(e, c, sending, action):
        sign = -1 if e < 2 else 1
        for d in ORDER:
            row_off = DIRECTIONS[d][0] * (sign if sending else -sign)
            if row_off == 0:
                action(copy(e, c, d))
            else:
                pl.when(there(row_off))(functools.partial(lambda e, c, d: action(copy(e, c, d)), e, c, d))

    def start(e, c):
        each(e, c, True, lambda item: item.start())

    def arrived(e, c):
        each(e, c, False, lambda item: item.wait_recv())

    def spread(wt_ref, cols_ref, mat, mat_t, base=0, count=extent):
        blocks, height, width = wt_ref.shape
        for b in range(blocks):
            index = cols_ref[b : b + 1, :]
            place_of = lax.broadcasted_iota(jnp.int32, (count, width), 0) + base
            hot = (place_of == index).astype(F32).astype(BF16)
            hi, lo = halves(wt_ref[b])
            span = pl.ds(b * height, height)
            if mat is not None:
                mat[0, span], mat[1, span] = halves(dot_nt(hi, hot) + dot_nt(lo, hot))
            if mat_t is not None:
                part = pl.ds(base, count)
                mat_t[0, part, span], mat_t[1, part, span] = halves(dot_nt(hot, hi) + dot_nt(hot, lo))

    def product(mat, row0, count, col0, depth, c, base):
        a_hi = mat[0, row0 : row0 + count, col0 : col0 + depth]
        a_lo = mat[1, row0 : row0 + count, col0 : col0 + depth]
        b_hi, b_lo = rhs[c][0, base : base + depth], rhs[c][1, base : base + depth]
        return dot(a_hi, b_hi) + (dot(a_hi, b_lo) + dot(a_lo, b_hi))

    def gathered(e, c):
        hi, lo = halves(recv[e][c][...])
        return dot(pick_t[...], hi) + dot(pick_t[...], lo)

    def place(c, base, value):
        rhs[c][0, base : base + value.shape[0]], rhs[c][1, base : base + value.shape[0]] = halves(value)

    def picked(c):
        return dot(pick[...], rhs[c][0, :n_own]) + dot(pick[...], rhs[c][1, :n_own])

    for e in range(4):
        sign = -1 if e < 2 else 1
        for d, (row_off, _) in enumerate(DIRECTIONS):
            if row_off:
                @pl.when(jnp.logical_not(there(-sign * row_off)))
                def _():
                    for c in range(n_chunks):
                        piece = recv[e][c].at[pl.ds(d * slot, slot)]
                        piece[...] = jnp.zeros(piece.shape, F32)

    loads[0].wait()
    spread(iwt_ref, icols_ref, None, imat_t, n_own, n_slot)
    limit = valid_ref[0, 0]
    edge = jnp.int32(2)
    edge += jnp.where(there(-1), 3, 0) + jnp.where(there(1), 3, 0)
    pl.semaphore_wait(barrier, edge)

    def keep(width):
        return lax.broadcasted_iota(jnp.int32, (rows, width), 0) < limit

    for c, (lo, width) in enumerate(chunks):
        loads[1 + c].wait()
        place(c, 0, jnp.where(keep(width), own[c][...], 0.0))
        send[0][c][...] = product(imat_t, n_own, n_slot, 0, rows, c, 0)
        start(0, c)
    spread(iwt_ref, icols_ref, None, imat_t, 0, n_own)
    for c in range(n_chunks):
        own[c][...] = product(imat_t, 0, n_own, 0, rows, c, 0)
    halo = jnp.concatenate([halo_ref[d : d + 1, :] for d in range(8)], axis=1)
    hot = (lax.broadcasted_iota(jnp.int32, (n_own, n_slot), 0) == halo).astype(F32)
    loads[-1].wait()
    pick_t[...] = hot.astype(BF16)
    pick[...] = hot.T.astype(BF16)
    spread(cwt_ref, ccols_ref, None, cmat_t)
    for c in range(n_chunks):
        arrived(0, c)
        place(c, 0, own[c][...] + gathered(0, c))
        send[1][c][...] = product(cmat_t, n_own, n_slot, 0, n_own, c, 0)
        start(1, c)
        own[c][...] = product(cmat_t, 0, n_own, 0, n_own, c, 0)
    spread(cwt_ref, ccols_ref, cmat, None)
    spread(iwt_ref, icols_ref, imat, None)
    for c in range(n_chunks):
        arrived(1, c)
        place(c, 0, own[c][...] + gathered(1, c))
        send[2][c][...] = picked(c)
        start(2, c)
        own[c][...] = product(cmat, 0, n_own, 0, n_own, c, 0)
    for c in range(n_chunks):
        arrived(2, c)
        place(c, n_own, recv[2][c][...])
        place(c, 0, own[c][...] + product(cmat, 0, n_own, n_own, n_slot, c, n_own))
        send[3][c][...] = picked(c)
        start(3, c)
        own[c][...] = product(imat, 0, rows, 0, n_own, c, 0)
    stores = []
    for c, (lo, width) in enumerate(chunks):
        arrived(3, c)
        place(c, n_own, recv[3][c][...])
        total = own[c][...] + product(imat, 0, rows, n_own, n_slot, c, n_own)
        own[c][...] = jnp.where(keep(width), total, 0.0)
        stores.append(
            pltpu.make_async_copy(own[c], out_ref.at[:, lo : lo + width], store_sem.at[c])
        )
        stores[c].start()
    for e in range(4):
        for c in range(n_chunks):
            each(e, c, True, lambda item: item.wait_send())
    for item in stores:
        item.wait()


def solution(mesh):
    n_ty, n_tx = mesh.shape["ty"], mesh.shape["tx"]

    def body(ctrl, interp_wt, interp_cols, conv_wt, conv_cols, halo_index, valid):
        rows, feat = ctrl.shape[2:]
        n_own = conv_wt.shape[2] * conv_wt.shape[3]
        n_slot = halo_index.shape[2] * halo_index.shape[3]
        extent = n_own + n_slot
        tiles = feat // 128
        first = 128 * max(tiles - tiles // 2, 1)
        chunks = ((0, first), (first, feat - first)) if feat > first else ((0, feat),)
        widths = [width for _, width in chunks]
        pin = functools.partial(pltpu.with_memory_space_constraint, memory_space=pltpu.HBM)
        hbm = pl.BlockSpec(memory_space=pltpu.HBM)
        vmem = pl.BlockSpec(memory_space=pltpu.VMEM)
        scratch = [
            pltpu.VMEM(interp_wt.shape[2:], F32),
            pltpu.VMEM(conv_wt.shape[2:], F32),
            pltpu.VMEM((2, rows, extent), BF16),
            pltpu.VMEM((2, extent, rows), BF16),
            pltpu.VMEM((2, n_own, extent), BF16),
            pltpu.VMEM((2, extent, n_own), BF16),
            pltpu.VMEM((n_slot, n_own), BF16),
            pltpu.VMEM((n_own, n_slot), BF16),
        ]
        assert rows == n_own
        scratch += [pltpu.VMEM((n_own, width), F32) for width in widths]
        scratch += [pltpu.VMEM((2, extent, width), BF16) for width in widths]
        scratch += [pltpu.VMEM((n_slot, width), F32) for _ in range(8) for width in widths]
        scratch += [pltpu.SemaphoreType.DMA((4, len(chunks), 8))] * 2
        scratch += [pltpu.SemaphoreType.DMA((2 + len(chunks),)), pltpu.SemaphoreType.DMA((len(chunks),))]
        out = pl.pallas_call(
            functools.partial(kernel, n_ty, n_tx, chunks),
            out_shape=jax.ShapeDtypeStruct((rows, feat), F32),
            in_specs=[pl.BlockSpec(memory_space=pltpu.SMEM), hbm, hbm, vmem, hbm, vmem, vmem],
            out_specs=pl.BlockSpec(memory_space=pl.ANY),
            scratch_shapes=scratch,
            compiler_params=pltpu.CompilerParams(
                collective_id=0, has_side_effects=True, vmem_limit_bytes=44 * 1024 * 1024
            ),
        )(
            valid, pin(ctrl[0, 0]), pin(interp_wt[0, 0]), pin(interp_cols[0, 0]), pin(conv_wt[0, 0]),
            pin(conv_cols[0, 0]), pin(halo_index[0, 0]),
        )
        return out[None, None]

    placed = (
        P("ty", "tx", None, None),
        P("ty", "tx", None, None, None),
        P("ty", "tx", None, None),
        P("ty", "tx", None, None, None),
        P("ty", "tx", None, None),
        P("ty", "tx", None, None),
        P("ty", "tx"),
    )
    return jax.shard_map(
        body, mesh=mesh, in_specs=placed, out_specs=P("ty", "tx", None, None), check_vma=False
    )
```
